512 devices in a mesh: dp: 128 (over z, x, y_hi, core), mp: 4 (over y_lo).
Axes of the slice: x: 4, y: 8 (y_hi: 2, y_lo: 4; y = y_hi * 4 + y_lo), z: 8, core: 2. Of those that a mesh axis runs over, the one named last changes fastest.
Arguments:
- factor_rows: bfloat16 [4, 128, 128, 768], P('mp', None, 'dp')
- old_statistic: float32 [128, 4, 768, 768], P('dp', 'mp'), may hold values from -1 to 2, as said below
- assignment: int32 [4, 128], P('mp'), may hold values from 0 to 127, each once within a row
- gradient: bfloat16 [128, 4, 768, 512], P('dp', None, None, 'mp'), may hold values from -3 to 3
Outputs:
- update: bfloat16 [128, 4, 768, 512], P('dp', None, None, 'mp')
The draws below stay inside these ranges and needn't reach their ends.
Inputs may be any that keep to these rules, and one draw needn't show every extreme that they name: Each row of assignment names every block number once. `old_statistic`: each block is symmetric positive definite.
All inputs are finite; a program needn't handle non-finite values.
Results may differ from the reference program's by a relative error of at most 0.001.
The reference program's roundings to bfloat16 on the way count: a program that leaves them out, or rounds other values in their place, can miss the bound.
Values may be sent and summed in bfloat16 or wider, within the bound.
A program may use at most 64 MiB of HBM per device.

```python
import math
import jax
import jax.numpy as jnp
from jax import lax

B = 768
COLS = 512
ROWS = 1
N_DP = 128
N_MP = 4


def draw_factor_rows(key, part):
    count = N_DP * ROWS
    shape = (N_MP, N_DP, count, B)
    key_base, key_scale = jax.random.split(jax.random.fold_in(key, 11), 2)
    base = jnp.clip(jax.random.normal(key_base, shape, jnp.float32), -6.0, 6.0)
    energy = jnp.exp(jax.random.uniform(key_scale, shape[:3] + (1,), jnp.float32, math.log(0.003), math.log(0.3)))
    scales = jnp.sqrt(energy * (count / B))
    return (base * scales).astype(jnp.bfloat16)


def draw_old_statistic(key, part):
    shape = (N_DP, N_MP, B, B)
    key_noise, key_diag = jax.random.split(jax.random.fold_in(key, 23))
    noise = jnp.clip(jax.random.normal(key_noise, shape, jnp.float32), -6.0, 6.0)
    noise = noise * (0.5 / math.sqrt(B))
    symmetric = 0.5 * (noise + jnp.swapaxes(noise, 2, 3))
    whole = jnp.eye(B, dtype=jnp.float32) + symmetric
    diagonal = 1.0 / jax.random.uniform(key_diag, shape[:3], jnp.float32, 1.0, float(B))
    roots = jnp.sqrt(diagonal)
    outer = roots[..., :, None] * roots[..., None, :]
    result = outer * whole
    return result


def shard_levels(stream_key, dims, pieces, least, high):
    level, own = 1.0, jax.random.fold_in(stream_key, 6)
    for dim, parts in pieces:
        steps = jnp.exp(jax.random.uniform(jax.random.fold_in(own, dim), (parts,), jnp.float32, least / len(pieces), high / len(pieces)))
        level = level * jnp.repeat(steps, dims[dim] // parts).reshape([-1 if axis == dim else 1 for axis in range(len(dims))])
    return level


def centred(stream_key, shape, deviation, reach, cuts=(), kind=jnp.bfloat16):
    factor_of = shard_levels(stream_key, shape, cuts, -0.22, 0.18) if cuts else 1.0
    values = jax.random.normal(stream_key, shape, jnp.float32) * deviation * factor_of
    return jnp.minimum(jnp.maximum(values, -reach), reach).astype(kind)


def setup_inputs(seed: int = 0) -> dict:
    key_list = jax.random.split(jax.random.key(seed), 5)
    factor_rows = draw_factor_rows(jax.random.fold_in(key_list[4], 71), 0)
    old_statistic = draw_old_statistic(jax.random.fold_in(key_list[4], 71), 0)
    assignment = jax.vmap(lambda own: jax.random.permutation(own, N_DP))(jax.random.split(key_list[2], N_MP)).reshape((N_MP, N_DP)).astype(jnp.int32)
    gradient = centred(key_list[3], (N_DP, N_MP, B, COLS), 0.5, 3.0, ((0, 128), (3, 4)))
    return {"factor_rows": factor_rows, "old_statistic": old_statistic, "assignment": assignment, "gradient": gradient}


def newton_factors(statistic):
    identity = jnp.eye(statistic.shape[0], dtype=jnp.float32)
    frob_norm = jnp.sqrt(jnp.sum(statistic * statistic) + 1e-06)
    normed = statistic / frob_norm
    step_one = ((5.0 * identity - normed) * 0.25).astype(jnp.bfloat16)
    square_one = jnp.dot(step_one, step_one, preferred_element_type=jnp.float32).astype(jnp.bfloat16)
    product_one = jnp.dot(square_one, normed.astype(jnp.bfloat16), preferred_element_type=jnp.float32).astype(jnp.bfloat16)
    coupled_one = jnp.dot(square_one, product_one, preferred_element_type=jnp.float32)
    step_two = ((5.0 * identity - coupled_one) * 0.25).astype(jnp.bfloat16)
    square_two = jnp.dot(step_two, step_two, preferred_element_type=jnp.float32).astype(jnp.bfloat16)
    product_two = jnp.dot(square_two, coupled_one.astype(jnp.bfloat16), preferred_element_type=jnp.float32).astype(jnp.bfloat16)
    coupled_two = jnp.dot(square_two, product_two, preferred_element_type=jnp.float32)
    step_three = ((5.0 * identity - coupled_two) / (4.0 * jnp.sqrt(jnp.sqrt(frob_norm)))).astype(jnp.bfloat16)
    return (step_one, step_two, step_three)

def apply_factors(step_one, step_two, step_three, block):
    first_pass = jnp.dot(step_three, block, preferred_element_type=jnp.float32).astype(jnp.bfloat16)
    second_pass = jnp.dot(step_two, first_pass, preferred_element_type=jnp.float32).astype(jnp.bfloat16)
    return jnp.dot(step_one, second_pass, preferred_element_type=jnp.float32).astype(jnp.bfloat16)

def reference(factor_rows, old_statistic, assignment, gradient):
    count = factor_rows.shape[2]

    def refresh_block(flat_index):
        owner_dp = flat_index // N_MP
        owner_mp = flat_index % N_MP
        block_id = assignment[owner_mp, owner_dp]
        factors = factor_rows[owner_mp, block_id]
        gram = lax.dot_general(factors, factors, (((0,), (0,)), ((), ())), preferred_element_type=jnp.float32)
        statistic = old_statistic[owner_dp, owner_mp] + gram / count
        step_one, step_two, step_three = newton_factors(statistic)
        return apply_factors(step_one, step_two, step_three, gradient[owner_dp, owner_mp])
    updated = lax.map(refresh_block, jnp.arange(N_DP * N_MP, dtype=jnp.int32))
    return updated.reshape(N_DP, N_MP, B, COLS)
```

```python
import jax
import jax.numpy as jnp
from jax import lax
from jax.experimental import pallas as pl
from jax.experimental.pallas import tpu as pltpu
from jax.sharding import PartitionSpec as P

MESH = pl.DeviceIdType.MESH
F32, BF16 = jnp.float32, jnp.bfloat16
TILE = 128
ROWS_PER = 8


def dot(a, b):
    return jnp.dot(a, b, preferred_element_type=F32)


def make_kernel(n_dp, n_mp, order):
    def kernel(
        rows_hbm, old_hbm, assign_hbm, grad_hbm, out_ref,
        rows, assign, stat, wide, sbuf, rbuf, gbuf, rbig,
        normed, step_one, step_two, step_three, square, product, coupled,
        load_sem, send_sem, recv_sem, gsend_sem, grecv_sem, osend_sem, orecv_sem, ready,
    ):
        size = stat.shape[0]
        n_cut = size // TILE
        me, mine = lax.axis_index("dp"), lax.axis_index("mp")

        def peer(d):
            return {"dp": d, "mp": mine}

        def group(m):
            return {"dp": me, "mp": m}

        barrier = pltpu.get_barrier_semaphore()

        def greet(d, carry):
            pl.semaphore_signal(barrier, inc=1, device_id=peer(d), device_id_type=MESH)
            return carry

        others = order(mine)
        for m in others:
            pl.semaphore_signal(barrier, inc=1, device_id=group(m), device_id_type=MESH)
        lax.fori_loop(me + 1, n_dp, greet, 0)

        loads = [
            pltpu.make_async_copy(assign_hbm, assign, load_sem.at[0]),
            pltpu.make_async_copy(rows_hbm, rows, load_sem.at[1]),
            pltpu.make_async_copy(old_hbm, stat, load_sem.at[2]),
            pltpu.make_async_copy(grad_hbm.at[mine], gbuf.at[mine], load_sem.at[3]),
        ]
        for load in loads:
            load.start()

        loads[0].wait()
        loads[1].wait()
        block = lax.broadcasted_iota(jnp.int32, (n_dp, n_dp), 0)
        hot = jnp.where(block == assign[...], 1.0, 0.0).astype(BF16)
        picked = lax.dot_general(
            hot, rows[...], (((0,), (0,)), ((), ())), preferred_element_type=F32
        )
        for j in range(n_cut):
            wide[pl.ds(j, n_dp, stride=ROWS_PER), :] = picked[:, j * TILE : (j + 1) * TILE]
        for j in range(n_cut, ROWS_PER):
            wide[pl.ds(j, n_dp, stride=ROWS_PER), :] = jnp.zeros((n_dp, TILE), F32)
        sbuf[...] = wide[...].astype(BF16).reshape(sbuf.shape)
        rbuf[me] = sbuf[me]

        pl.semaphore_wait(barrier, me + len(others))

        def send(d):
            pltpu.make_async_remote_copy(
                sbuf.at[d], rbuf.at[me], send_sem.at[0], recv_sem.at[0],
                device_id=peer(d), device_id_type=MESH,
            ).start()

        def earlier(d, carry):
            pl.semaphore_signal(ready.at[me], inc=1, device_id=peer(d), device_id_type=MESH)
            send(d)
            return carry

        lax.fori_loop(0, me, earlier, 0)

        arriving = []
        for k, m in enumerate(others):
            copy = pltpu.make_async_remote_copy(
                grad_hbm.at[m], gbuf.at[mine], gsend_sem.at[k], grecv_sem.at[mine],
                device_id=group(m), device_id_type=MESH,
            )
            copy.start()
            arriving.append(copy)

        def later(d, carry):
            pl.semaphore_wait(ready.at[d], 1)
            send(d)
            return carry

        lax.fori_loop(me + 1, n_dp, later, 0)

        all_but_one = rbuf.at[pl.ds(0, n_dp - 1)]
        pltpu.make_async_copy(all_but_one, all_but_one, recv_sem.at[0]).wait()
        wide[...] = rbuf[...].reshape(wide.shape).astype(F32)
        for j in range(n_cut):
            rbig[:, j * TILE : (j + 1) * TILE] = wide[
                pl.ds(j, n_dp, stride=ROWS_PER), :
            ].astype(BF16)

        loads[2].wait()
        step = 256
        cuts = [slice(i, i + step) for i in range(0, size, step)]
        total = jnp.zeros((), F32)
        for cut in cuts:
            gram = lax.dot_general(
                rbig[:, cut], rbig[...], (((0,), (0,)), ((), ())), preferred_element_type=F32
            )
            value = stat[cut, :] + gram * (1.0 / n_dp)
            stat[cut, :] = value
            total = total + jnp.sum(value * value)
        frob = jnp.sqrt(total + 1e-06)
        inverse = 1.0 / frob
        last_scale = 1.0 / (4.0 * jnp.sqrt(jnp.sqrt(frob)))

        def diagonal(cut):
            down = lax.broadcasted_iota(jnp.int32, (step, size), 0) + cut.start
            across = lax.broadcasted_iota(jnp.int32, (step, size), 1)
            return jnp.where(down == across, 5.0, 0.0).astype(F32)

        for cut in cuts:
            value = stat[cut, :] * inverse
            normed[cut, :] = value.astype(BF16)
            step_one[cut, :] = ((diagonal(cut) - value) * 0.25).astype(BF16)
        for cut in cuts:
            square[cut, :] = dot(step_one[cut, :], step_one[...]).astype(BF16)
        for cut in cuts:
            product[cut, :] = dot(square[cut, :], normed[...]).astype(BF16)
        for cut in cuts:
            value = dot(square[cut, :], product[...])
            coupled[cut, :] = value.astype(BF16)
            step_two[cut, :] = ((diagonal(cut) - value) * 0.25).astype(BF16)
        for cut in cuts:
            square[cut, :] = dot(step_two[cut, :], step_two[...]).astype(BF16)
        for cut in cuts:
            product[cut, :] = dot(square[cut, :], coupled[...]).astype(BF16)
        for cut in cuts:
            value = dot(square[cut, :], product[...])
            step_three[cut, :] = ((diagonal(cut) - value) * last_scale).astype(BF16)

        loads[3].wait()

        def arrived(m):
            spot = gbuf.at[m]
            pltpu.make_async_copy(spot, spot, grecv_sem.at[m]).wait()

        def applied(first, second):
            block = jnp.concatenate([gbuf[first], gbuf[second]], axis=1)
            one = dot(step_three[...], block).astype(BF16)
            two = dot(step_two[...], one).astype(BF16)
            three = dot(step_one[...], two).astype(BF16)
            gbuf[first] = three[:, :TILE]
            gbuf[second] = three[:, TILE:]

        leaving = []

        def leave(k, m):
            copy = pltpu.make_async_remote_copy(
                gbuf.at[m], out_ref.at[mine], osend_sem.at[k], orecv_sem.at[mine],
                device_id=group(m), device_id_type=MESH,
            )
            copy.start()
            leaving.append(copy)

        arrived(others[0])
        arrived(others[1])
        applied(others[0], others[1])
        leave(0, others[0])
        leave(1, others[1])
        arrived(others[2])
        applied(others[2], mine)
        leave(2, others[2])
        stay = pltpu.make_async_copy(gbuf.at[mine], out_ref.at[mine], load_sem.at[3])
        stay.start()
        for copy in arriving:
            copy.wait_send()
        sent = sbuf.at[pl.ds(0, n_dp - 1)]
        pltpu.make_async_copy(sent, sent, send_sem.at[0]).wait()
        stay.wait()
        for copy in leaving:
            copy.wait_send()
        for m in others:
            spot = out_ref.at[m]
            pltpu.make_async_copy(spot, spot, orecv_sem.at[m]).wait()

    return kernel


def solution(mesh):
    n_dp, n_mp = mesh.shape["dp"], mesh.shape["mp"]

    def order(m):
        near = 1 + lax.rem(m, 2)
        far = jnp.where(m < 2, 3, 0)
        return near, 6 - m - near - far, far

    def body(factor_rows, old_statistic, assignment, gradient):
        size, cols = gradient.shape[2:]
        any_spec = pl.BlockSpec(memory_space=pl.ANY)
        square = pltpu.VMEM((size, size), BF16)
        result = pl.pallas_call(
            make_kernel(n_dp, n_mp, order),
            out_shape=jax.ShapeDtypeStruct((n_mp, size, cols), BF16),
            in_specs=[any_spec] * 4,
            out_specs=any_spec,
            scratch_shapes=[
                pltpu.VMEM((n_dp, size), BF16),
                pltpu.VMEM((1, n_dp), jnp.int32),
                pltpu.VMEM((size, size), F32),
                pltpu.VMEM((n_dp * ROWS_PER, TILE), F32),
                pltpu.VMEM((n_dp, ROWS_PER, TILE), BF16),
                pltpu.VMEM((n_dp, ROWS_PER, TILE), BF16),
                pltpu.VMEM((n_mp, size, cols), BF16),
                pltpu.VMEM((n_dp, size), BF16),
                square, square, square, square, square, square, square,
                pltpu.SemaphoreType.DMA((4,)),
                pltpu.SemaphoreType.DMA((1,)),
                pltpu.SemaphoreType.DMA((1,)),
                pltpu.SemaphoreType.DMA((n_mp - 1,)),
                pltpu.SemaphoreType.DMA((n_mp,)),
                pltpu.SemaphoreType.DMA((n_mp - 1,)),
                pltpu.SemaphoreType.DMA((n_mp,)),
                pltpu.SemaphoreType.REGULAR((n_dp,)),
            ],
            compiler_params=pltpu.CompilerParams(
                collective_id=0, has_side_effects=True, vmem_limit_bytes=48 * 1024 * 1024
            ),
        )(
            factor_rows.reshape(n_dp, size),
            old_statistic.reshape(size, size),
            assignment,
            gradient.reshape(n_mp, size, cols),
        )
        return result.reshape(gradient.shape)

    return jax.shard_map(
        body,
        mesh=mesh,
        in_specs=(
            P("mp", None, "dp", None),
            P("dp", "mp", None, None),
            P("mp", None),
            P("dp", None, None, "mp"),
        ),
        out_specs=P("dp", None, None, "mp"),
        check_vma=False,
    )
```

```python
import jax
import jax.numpy as jnp
from jax import lax
from jax.experimental import pallas as pl
from jax.experimental.pallas import tpu as pltpu
from jax.sharding import PartitionSpec as P

MESH = pl.DeviceIdType.MESH
F32, BF16 = jnp.float32, jnp.bfloat16
TILE = 128
ROWS_PER = 8


def dot(a, b):
    return jnp.dot(a, b, preferred_element_type=F32)


def make_kernel(n_dp, n_mp, order):
    def kernel(
        rows_hbm, old_hbm, assign_hbm, grad_hbm, out_ref,
        rows, assign, stat, wide, sbuf, rbuf, gbuf, rbig,
        normed, step_one, step_two, step_three, square, product, coupled,
        load_sem, send_sem, recv_sem, gsend_sem, grecv_sem, osend_sem, orecv_sem, ready,
    ):
        size = stat.shape[0]
        n_cut = size // TILE
        me, mine = lax.axis_index("dp"), lax.axis_index("mp")

        def peer(d):
            return {"dp": d, "mp": mine}

        def group(m):
            return {"dp": me, "mp": m}

        barrier = pltpu.get_barrier_semaphore()

        def greet(d, carry):
            pl.semaphore_signal(barrier, inc=1, device_id=peer(d), device_id_type=MESH)
            return carry

        loads = [
            pltpu.make_async_copy(assign_hbm, assign, load_sem.at[0]),
            pltpu.make_async_copy(rows_hbm, rows, load_sem.at[1]),
            pltpu.make_async_copy(old_hbm, stat, load_sem.at[2]),
            pltpu.make_async_copy(grad_hbm.at[mine], gbuf.at[mine], load_sem.at[3]),
        ]
        for load in loads:
            load.start()

        others = order(mine)
        for m in others:
            pl.semaphore_signal(barrier, inc=1, device_id=group(m), device_id_type=MESH)
        lax.fori_loop(me + 1, n_dp, greet, 0)

        loads[0].wait()
        loads[1].wait()
        block = lax.broadcasted_iota(jnp.int32, (n_dp, n_dp), 0)
        hot = jnp.where(block == assign[...], 1.0, 0.0).astype(BF16)
        picked = lax.dot_general(
            hot, rows[...], (((0,), (0,)), ((), ())), preferred_element_type=F32
        )
        for j in range(n_cut):
            wide[pl.ds(j, n_dp, stride=ROWS_PER), :] = picked[:, j * TILE : (j + 1) * TILE]
        for j in range(n_cut, ROWS_PER):
            wide[pl.ds(j, n_dp, stride=ROWS_PER), :] = jnp.zeros((n_dp, TILE), F32)
        sbuf[...] = wide[...].astype(BF16).reshape(sbuf.shape)
        rbuf[me] = sbuf[me]

        pl.semaphore_wait(barrier, me + len(others))

        def send(d):
            pltpu.make_async_remote_copy(
                sbuf.at[d, pl.ds(0, n_cut)], rbuf.at[me, pl.ds(0, n_cut)], send_sem.at[0], recv_sem.at[0],
                device_id=peer(d), device_id_type=MESH,
            ).start()

        def earlier(d, carry):
            pl.semaphore_signal(ready.at[me], inc=1, device_id=peer(d), device_id_type=MESH)
            send(d)
            return carry

        lax.fori_loop(0, me, earlier, 0)

        arriving = []
        for k, m in enumerate(others):
            copy = pltpu.make_async_remote_copy(
                grad_hbm.at[m], gbuf.at[mine], gsend_sem.at[k], grecv_sem.at[mine],
                device_id=group(m), device_id_type=MESH,
            )
            copy.start()
            arriving.append(copy)

        def later(d, carry):
            pl.semaphore_wait(ready.at[d], 1)
            send(d)
            return carry

        lax.fori_loop(me + 1, n_dp, later, 0)

        all_but_one = rbuf.at[pl.ds(0, n_dp - 1), pl.ds(0, n_cut)]
        pltpu.make_async_copy(all_but_one, all_but_one, recv_sem.at[0]).wait()
        wide[...] = rbuf[...].reshape(wide.shape).astype(F32)
        for j in range(n_cut):
            rbig[:, j * TILE : (j + 1) * TILE] = wide[
                pl.ds(j, n_dp, stride=ROWS_PER), :
            ].astype(BF16)

        loads[2].wait()
        step = 256
        cuts = [slice(i, i + step) for i in range(0, size, step)]
        total = jnp.zeros((), F32)
        for cut in cuts:
            gram = lax.dot_general(
                rbig[:, cut], rbig[...], (((0,), (0,)), ((), ())), preferred_element_type=F32
            )
            value = stat[cut, :] + gram * (1.0 / n_dp)
            stat[cut, :] = value
            total = total + jnp.sum(value * value)
        frob = jnp.sqrt(total + 1e-06)
        inverse = 1.0 / frob
        last_scale = 1.0 / (4.0 * jnp.sqrt(jnp.sqrt(frob)))

        def diagonal(cut):
            down = lax.broadcasted_iota(jnp.int32, (step, size), 0) + cut.start
            across = lax.broadcasted_iota(jnp.int32, (step, size), 1)
            return jnp.where(down == across, 5.0, 0.0).astype(F32)

        for cut in cuts:
            value = stat[cut, :] * inverse
            normed[cut, :] = value.astype(BF16)
            step_one[cut, :] = ((diagonal(cut) - value) * 0.25).astype(BF16)
        for cut in cuts:
            square[cut, :] = dot(step_one[cut, :], step_one[...]).astype(BF16)
        for cut in cuts:
            product[cut, :] = dot(square[cut, :], normed[...]).astype(BF16)
        for cut in cuts:
            value = dot(square[cut, :], product[...])
            coupled[cut, :] = value.astype(BF16)
            step_two[cut, :] = ((diagonal(cut) - value) * 0.25).astype(BF16)
        for cut in cuts:
            square[cut, :] = dot(step_two[cut, :], step_two[...]).astype(BF16)
        for cut in cuts:
            product[cut, :] = dot(square[cut, :], coupled[...]).astype(BF16)
        for cut in cuts:
            value = dot(square[cut, :], product[...])
            step_three[cut, :] = ((diagonal(cut) - value) * last_scale).astype(BF16)

        loads[3].wait()

        def arrived(m):
            spot = gbuf.at[m]
            pltpu.make_async_copy(spot, spot, grecv_sem.at[m]).wait()

        def applied(first, second):
            block = jnp.concatenate([gbuf[first], gbuf[second]], axis=1)
            one = dot(step_three[...], block).astype(BF16)
            two = dot(step_two[...], one).astype(BF16)
            three = dot(step_one[...], two).astype(BF16)
            gbuf[first] = three[:, :TILE]
            gbuf[second] = three[:, TILE:]

        leaving = []

        def leave(k, m):
            copy = pltpu.make_async_remote_copy(
                gbuf.at[m], out_ref.at[mine], osend_sem.at[k], orecv_sem.at[mine],
                device_id=group(m), device_id_type=MESH,
            )
            copy.start()
            leaving.append(copy)

        arrived(others[0])
        arrived(others[1])
        applied(others[0], others[1])
        leave(0, others[0])
        leave(1, others[1])
        arrived(others[2])
        applied(others[2], mine)
        leave(2, others[2])
        stay = pltpu.make_async_copy(gbuf.at[mine], out_ref.at[mine], load_sem.at[3])
        stay.start()
        for copy in arriving:
            copy.wait_send()
        sent = sbuf.at[pl.ds(0, n_dp - 1), pl.ds(0, n_cut)]
        pltpu.make_async_copy(sent, sent, send_sem.at[0]).wait()
        stay.wait()
        for copy in leaving:
            copy.wait_send()
        for m in others:
            spot = out_ref.at[m]
            pltpu.make_async_copy(spot, spot, orecv_sem.at[m]).wait()

    return kernel


def solution(mesh):
    n_dp, n_mp = mesh.shape["dp"], mesh.shape["mp"]

    def order(m):
        near = 1 + lax.rem(m, 2)
        far = jnp.where(m < 2, 3, 0)
        return near, 6 - m - near - far, far

    def body(factor_rows, old_statistic, assignment, gradient):
        size, cols = gradient.shape[2:]
        any_spec = pl.BlockSpec(memory_space=pl.ANY)
        square = pltpu.VMEM((size, size), BF16)
        result = pl.pallas_call(
            make_kernel(n_dp, n_mp, order),
            out_shape=jax.ShapeDtypeStruct((n_mp, size, cols), BF16),
            in_specs=[any_spec] * 4,
            out_specs=any_spec,
            scratch_shapes=[
                pltpu.VMEM((n_dp, size), BF16),
                pltpu.VMEM((1, n_dp), jnp.int32),
                pltpu.VMEM((size, size), F32),
                pltpu.VMEM((n_dp * ROWS_PER, TILE), F32),
                pltpu.VMEM((n_dp, ROWS_PER, TILE), BF16),
                pltpu.VMEM((n_dp, ROWS_PER, TILE), BF16),
                pltpu.VMEM((n_mp, size, cols), BF16),
                pltpu.VMEM((n_dp, size), BF16),
                square, square, square, square, square, square, square,
                pltpu.SemaphoreType.DMA((4,)),
                pltpu.SemaphoreType.DMA((1,)),
                pltpu.SemaphoreType.DMA((1,)),
                pltpu.SemaphoreType.DMA((n_mp - 1,)),
                pltpu.SemaphoreType.DMA((n_mp,)),
                pltpu.SemaphoreType.DMA((n_mp - 1,)),
                pltpu.SemaphoreType.DMA((n_mp,)),
                pltpu.SemaphoreType.REGULAR((n_dp,)),
            ],
            compiler_params=pltpu.CompilerParams(
                collective_id=0, has_side_effects=True, vmem_limit_bytes=66000000
            ),
        )(
            factor_rows.reshape(n_dp, size),
            old_statistic.reshape(size, size),
            assignment,
            gradient.reshape(n_mp, size, cols),
        )
        return result.reshape(gradient.shape)

    return jax.shard_map(
        body,
        mesh=mesh,
        in_specs=(
            P("mp", None, "dp", None),
            P("dp", "mp", None, None),
            P("mp", None),
            P("dp", None, None, "mp"),
        ),
        out_specs=P("dp", None, None, "mp"),
        check_vma=False,
    )
```

```python
import jax
import jax.numpy as jnp
from jax import lax
from jax.experimental import pallas as pl
from jax.experimental.pallas import tpu as pltpu
from jax.sharding import PartitionSpec as P

MESH = pl.DeviceIdType.MESH
F32, BF16 = jnp.float32, jnp.bfloat16
TILE = 128
ROWS_PER = 8


def dot(a, b):
    return jnp.dot(a, b, preferred_element_type=F32)


def make_kernel(n_dp, n_mp, order):
    def kernel(
        rows_hbm, old_hbm, assign_hbm, grad_hbm, out_ref,
        rows, assign, stat, wide, sbuf, rbuf, gbuf, rbig,
        normed, step_one, step_two, step_three, square, product, coupled,
        load_sem, send_sem, recv_sem, gsend_sem, grecv_sem, osend_sem, orecv_sem, ready,
    ):
        size = stat.shape[0]
        n_cut = size // TILE
        me, mine = lax.axis_index("dp"), lax.axis_index("mp")

        def peer(d):
            return {"dp": d, "mp": mine}

        def group(m):
            return {"dp": me, "mp": m}

        barrier = pltpu.get_barrier_semaphore()

        def greet(d, carry):
            pl.semaphore_signal(barrier, inc=1, device_id=peer(d), device_id_type=MESH)
            return carry

        loads = [
            pltpu.make_async_copy(assign_hbm, assign, load_sem.at[0]),
            pltpu.make_async_copy(rows_hbm, rows, load_sem.at[1]),
            pltpu.make_async_copy(old_hbm, stat, load_sem.at[2]),
            pltpu.make_async_copy(grad_hbm.at[mine], gbuf.at[mine], load_sem.at[3]),
        ]
        for load in loads:
            load.start()

        others = order(mine)
        for m in others:
            pl.semaphore_signal(barrier, inc=1, device_id=group(m), device_id_type=MESH)
        lax.fori_loop(me + 1, n_dp, greet, 0)

        loads[0].wait()
        loads[1].wait()
        block = lax.broadcasted_iota(jnp.int32, (n_dp, n_dp), 0)
        hot = jnp.where(block == assign[...], 1.0, 0.0).astype(BF16)
        picked = lax.dot_general(
            hot, rows[...], (((0,), (0,)), ((), ())), preferred_element_type=F32
        )
        for j in range(n_cut):
            wide[pl.ds(j, n_dp, stride=ROWS_PER), :] = picked[:, j * TILE : (j + 1) * TILE]
        for j in range(n_cut, ROWS_PER):
            wide[pl.ds(j, n_dp, stride=ROWS_PER), :] = jnp.zeros((n_dp, TILE), F32)
        sbuf[...] = wide[...].astype(BF16).reshape(sbuf.shape)
        rbuf[me] = sbuf[me]

        pl.semaphore_wait(barrier, me + len(others))

        def send(d):
            pltpu.make_async_remote_copy(
                sbuf.at[d, pl.ds(0, n_cut)], rbuf.at[me, pl.ds(0, n_cut)], send_sem.at[0], recv_sem.at[0],
                device_id=peer(d), device_id_type=MESH,
            ).start()

        def earlier(d, carry):
            pl.semaphore_signal(ready.at[me], inc=1, device_id=peer(d), device_id_type=MESH)
            send(d)
            return carry

        lax.fori_loop(0, me, earlier, 0)

        arriving = []

        def share(k):
            copy = pltpu.make_async_remote_copy(
                grad_hbm.at[others[k]], gbuf.at[mine], gsend_sem.at[k], grecv_sem.at[mine],
                device_id=group(others[k]), device_id_type=MESH,
            )
            copy.start()
            arriving.append(copy)

        share(0)
        share(1)

        def later(d, carry):
            pl.semaphore_wait(ready.at[d], 1)
            send(d)
            return carry

        lax.fori_loop(me + 1, n_dp, later, 0)
        share(2)

        all_but_one = rbuf.at[pl.ds(0, n_dp - 1), pl.ds(0, n_cut)]
        pltpu.make_async_copy(all_but_one, all_but_one, recv_sem.at[0]).wait()
        wide[...] = rbuf[...].reshape(wide.shape).astype(F32)
        for j in range(n_cut):
            rbig[:, j * TILE : (j + 1) * TILE] = wide[
                pl.ds(j, n_dp, stride=ROWS_PER), :
            ].astype(BF16)

        loads[2].wait()
        step = 256
        cuts = [slice(i, i + step) for i in range(0, size, step)]
        total = jnp.zeros((), F32)
        for cut in cuts:
            gram = lax.dot_general(
                rbig[:, cut], rbig[...], (((0,), (0,)), ((), ())), preferred_element_type=F32
            )
            value = stat[cut, :] + gram * (1.0 / n_dp)
            stat[cut, :] = value
            total = total + jnp.sum(value * value)
        frob = jnp.sqrt(total + 1e-06)
        inverse = 1.0 / frob
        last_scale = 1.0 / (4.0 * jnp.sqrt(jnp.sqrt(frob)))

        def diagonal(cut):
            down = lax.broadcasted_iota(jnp.int32, (step, size), 0) + cut.start
            across = lax.broadcasted_iota(jnp.int32, (step, size), 1)
            return jnp.where(down == across, 5.0, 0.0).astype(F32)

        for cut in cuts:
            value = stat[cut, :] * inverse
            normed[cut, :] = value.astype(BF16)
            step_one[cut, :] = ((diagonal(cut) - value) * 0.25).astype(BF16)
        for cut in cuts:
            square[cut, :] = dot(step_one[cut, :], step_one[...]).astype(BF16)
        for cut in cuts:
            product[cut, :] = dot(square[cut, :], normed[...]).astype(BF16)
        for cut in cuts:
            value = dot(square[cut, :], product[...])
            coupled[cut, :] = value.astype(BF16)
            step_two[cut, :] = ((diagonal(cut) - value) * 0.25).astype(BF16)
        for cut in cuts:
            square[cut, :] = dot(step_two[cut, :], step_two[...]).astype(BF16)
        for cut in cuts:
            product[cut, :] = dot(square[cut, :], coupled[...]).astype(BF16)
        for cut in cuts:
            value = dot(square[cut, :], product[...])
            step_three[cut, :] = ((diagonal(cut) - value) * last_scale).astype(BF16)

        loads[3].wait()

        def arrived(m):
            spot = gbuf.at[m]
            pltpu.make_async_copy(spot, spot, grecv_sem.at[m]).wait()

        def applied(first, second):
            block = jnp.concatenate([gbuf[first], gbuf[second]], axis=1)
            one = dot(step_three[...], block).astype(BF16)
            two = dot(step_two[...], one).astype(BF16)
            three = dot(step_one[...], two).astype(BF16)
            gbuf[first] = three[:, :TILE]
            gbuf[second] = three[:, TILE:]

        leaving = []

        def leave(k, m):
            copy = pltpu.make_async_remote_copy(
                gbuf.at[m], out_ref.at[mine], osend_sem.at[k], orecv_sem.at[mine],
                device_id=group(m), device_id_type=MESH,
            )
            copy.start()
            leaving.append(copy)

        arrived(others[0])
        arrived(others[1])
        applied(others[0], others[1])
        leave(0, others[0])
        leave(1, others[1])
        arrived(others[2])
        applied(others[2], mine)
        leave(2, others[2])
        stay = pltpu.make_async_copy(gbuf.at[mine], out_ref.at[mine], load_sem.at[3])
        stay.start()
        for copy in arriving:
            copy.wait_send()
        sent = sbuf.at[pl.ds(0, n_dp - 1), pl.ds(0, n_cut)]
        pltpu.make_async_copy(sent, sent, send_sem.at[0]).wait()
        stay.wait()
        for copy in leaving:
            copy.wait_send()
        for m in others:
            spot = out_ref.at[m]
            pltpu.make_async_copy(spot, spot, orecv_sem.at[m]).wait()

    return kernel


def solution(mesh):
    n_dp, n_mp = mesh.shape["dp"], mesh.shape["mp"]

    def order(m):
        near = 1 + lax.rem(m, 2)
        far = jnp.where(m < 2, 3, 0)
        return near, 6 - m - near - far, far

    def body(factor_rows, old_statistic, assignment, gradient):
        size, cols = gradient.shape[2:]
        any_spec = pl.BlockSpec(memory_space=pl.ANY)
        square = pltpu.VMEM((size, size), BF16)
        result = pl.pallas_call(
            make_kernel(n_dp, n_mp, order),
            out_shape=jax.ShapeDtypeStruct((n_mp, size, cols), BF16),
            in_specs=[any_spec] * 4,
            out_specs=any_spec,
            scratch_shapes=[
                pltpu.VMEM((n_dp, size), BF16),
                pltpu.VMEM((1, n_dp), jnp.int32),
                pltpu.VMEM((size, size), F32),
                pltpu.VMEM((n_dp * ROWS_PER, TILE), F32),
                pltpu.VMEM((n_dp, ROWS_PER, TILE), BF16),
                pltpu.VMEM((n_dp, ROWS_PER, TILE), BF16),
                pltpu.VMEM((n_mp, size, cols), BF16),
                pltpu.VMEM((n_dp, size), BF16),
                square, square, square, square, square, square, square,
                pltpu.SemaphoreType.DMA((4,)),
                pltpu.SemaphoreType.DMA((1,)),
                pltpu.SemaphoreType.DMA((1,)),
                pltpu.SemaphoreType.DMA((n_mp - 1,)),
                pltpu.SemaphoreType.DMA((n_mp,)),
                pltpu.SemaphoreType.DMA((n_mp - 1,)),
                pltpu.SemaphoreType.DMA((n_mp,)),
                pltpu.SemaphoreType.REGULAR((n_dp,)),
            ],
            compiler_params=pltpu.CompilerParams(
                collective_id=0, has_side_effects=True, vmem_limit_bytes=66000000
            ),
        )(
            factor_rows.reshape(n_dp, size),
            old_statistic.reshape(size, size),
            assignment,
            gradient.reshape(n_mp, size, cols),
        )
        return result.reshape(gradient.shape)

    return jax.shard_map(
        body,
        mesh=mesh,
        in_specs=(
            P("mp", None, "dp", None),
            P("dp", "mp", None, None),
            P("mp", None),
            P("dp", None, None, "mp"),
        ),
        out_specs=P("dp", None, None, "mp"),
        check_vma=False,
    )
```
